32 devices in a mesh: atom: 4 (over y, x), tm: 8 (over z, core).
Axes of the slice: x: 2, y: 2, z: 4, core: 2. Of those that a mesh axis runs over, the one named last changes fastest.
Arguments:
- signal: bfloat16 [306, 8192], P(None, 'tm'), may hold values from -6 to 6
- spatial: bfloat16 [256, 306], P('atom'), may hold values from -0.3125 to 0.3125
- temporal: bfloat16 [256, 256], P('atom'), may hold values from -0.375 to 0.375
- code_values: bfloat16 [256, 8192], P('atom', 'tm'), may hold values from 0 to 2
- block_mask: int32 [256, 32], P('atom', 'tm'), may hold values 0 or 1
Outputs:
- grad_spatial: float32 [256, 306], P('atom')
- grad_temporal: float32 [256, 256], P('atom')
The draws below stay inside these ranges and needn't reach their ends.
All inputs are finite; a program needn't handle non-finite values. No bound on the sum of `block_mask` on one device may be relied on, other than what follows from the above.
Results may differ from the reference program's by a relative error of at most 0.0025.
Values may be sent and summed in bfloat16 or wider, within the bound.
A program may use at most 64 MiB of HBM per device.

```python
import math
import jax
import jax.numpy as jnp
from jax import lax

K = 256
P_SIZE = 306
L = 256
TIME = 8192
NBLK = 32
N_ATOM = 4


def place_ends(drawn, own_key, smallest, largest):
    index_at = [jax.random.randint(jax.random.fold_in(own_key, axis), (), 0, length) for axis, length in enumerate(drawn.shape)]
    main_axis = drawn.shape.index(max(drawn.shape))
    beside = index_at[:main_axis] + [(index_at[main_axis] + 1) % drawn.shape[main_axis]] + index_at[main_axis + 1:]
    return drawn.at[tuple(index_at)].set(smallest).at[tuple(beside)].set(largest)


def level_of(stream_key, dims, shards, low, largest):
    level, own = 1.0, jax.random.fold_in(stream_key, 6)
    for axis_at, blocks in shards:
        draws = jnp.exp(jax.random.uniform(jax.random.fold_in(own, axis_at), (blocks,), jnp.float32, low / len(shards), largest / len(shards)))
        level = level * jnp.repeat(draws, dims[axis_at] // blocks).reshape([-1 if axis == axis_at else 1 for axis in range(len(dims))])
    return level


def gaussian(key, extent, spread, bound, cuts=(), kind=jnp.bfloat16):
    result = spread * jax.random.normal(key, extent, jnp.float32)
    if cuts:
        result = result * level_of(key, extent, cuts, -0.22, 0.18)
    return jnp.clip(result, -bound, bound).astype(kind)


def setup_inputs(seed: int = 0) -> dict:
    streams_of = jax.random.split(jax.random.key(seed), 6)
    return {
        "signal": gaussian(streams_of[0], (P_SIZE, TIME), 1.0, 6.0, ((1, 8),)),
        "spatial": gaussian(streams_of[1], (K, P_SIZE), P_SIZE ** -0.5, 0.3125, ((0, 4),)),
        "temporal": gaussian(streams_of[2], (K, L), L ** -0.5, 0.375, ((0, 4),)),
        "code_values": jnp.clip(2.0 * jax.random.uniform(streams_of[3], (K, TIME), jnp.float32) ** level_of(streams_of[3], (K, TIME), ((0, 4), (1, 8)), -0.2, 0.2), 0.0, 2.0).astype(jnp.bfloat16),
        "block_mask": place_ends((jax.random.randint(streams_of[4], (K, NBLK), 0, 3) < 1).astype(jnp.int32), jax.random.fold_in(streams_of[4], 1), 0, 1),
    }


def toeplitz(kernels):
    count, length = kernels.shape
    heads = jnp.concatenate([jnp.zeros((count, 2 * length), kernels.dtype), kernels], axis=1)
    tiled = jnp.tile(heads, (1, 2 * length))[:, :2 * length * (3 * length - 1)]
    return tiled.reshape(count, 2 * length, 3 * length - 1)[:, :, :length]

def diagonals(products):
    count, rows_all, length = products.shape
    padded = jnp.concatenate([jnp.zeros((count, rows_all, 2 * length), products.dtype), products], axis=2)
    padded = padded.reshape(count, rows_all * 3 * length)
    padded = jnp.concatenate([padded, jnp.zeros((count, rows_all), products.dtype)], axis=1)
    skewed = padded.reshape(count, rows_all, 3 * length + 1)
    return lax.optimization_barrier(jnp.sum(skewed, axis=1))[:, length:2 * length]

def windows_of(extended, length):
    count, total = extended.shape
    blocks = extended.reshape(count, total // length, length)
    return jnp.concatenate([blocks[:, :-1], blocks[:, 1:]], axis=2)

def reference(signal, spatial, temporal, code_values, block_mask):
    atoms, channels = spatial.shape
    length = temporal.shape[1]
    samples = signal.shape[1]
    nblocks = samples // length
    groups = atoms // 4
    codes = (code_values.reshape(atoms, nblocks, length) * block_mask[:, :, None].astype(code_values.dtype)).reshape(atoms, samples)
    extended = jnp.concatenate([jnp.zeros((atoms, length), codes.dtype), codes], axis=1)

    def forward_group(operands):
        ext_group, kernels = operands
        windows = windows_of(ext_group, length).astype(jnp.float32)
        matrix = toeplitz(kernels).astype(jnp.float32)
        course_group = jnp.einsum('gbm,gms->gbs', windows, matrix)
        return course_group.reshape(4, samples).astype(jnp.bfloat16)
    course = lax.map(forward_group, (extended.reshape(groups, 4, length + samples), temporal.reshape(groups, 4, length)))
    course = course.reshape(atoms, samples)
    per_device = atoms // N_ATOM

    def add_group(total, operands):
        spatial_group, course_group = operands
        part = jnp.dot(spatial_group.T, course_group, preferred_element_type=jnp.float32).astype(jnp.bfloat16)
        part = lax.optimization_barrier(part)
        return (total + part.astype(jnp.float32), None)
    model, _ = lax.scan(add_group, jnp.zeros((channels, samples), jnp.float32), (spatial.reshape(N_ATOM, per_device, channels), course.reshape(N_ATOM, per_device, samples)))
    residual = (model - signal.astype(jnp.float32)).astype(jnp.bfloat16)
    projected = jnp.dot(spatial, residual, preferred_element_type=jnp.float32).astype(jnp.bfloat16)
    factor = 1.0 / math.sqrt(samples)
    grad_spatial = lax.dot_general(course, residual, (((1,), (1,)), ((), ())), preferred_element_type=jnp.float32) * factor

    def adjoint_group(operands):
        ext_group, proj_group = operands
        windows = windows_of(ext_group, length).astype(jnp.float32)
        proj_blocks = proj_group.reshape(4, nblocks, length).astype(jnp.float32)
        products = jnp.einsum('gbm,gbs->gms', windows, proj_blocks)
        return diagonals(products)
    grad_temporal = lax.map(adjoint_group, (extended.reshape(groups, 4, length + samples), projected.reshape(groups, 4, samples)))
    grad_temporal = grad_temporal.reshape(atoms, length) * factor
    return (grad_spatial, grad_temporal)
```

```python
import functools
import math

import jax
import jax.numpy as jnp
from jax import lax
from jax.experimental import pallas as pl
from jax.experimental.pallas import tpu as pltpu
from jax.sharding import PartitionSpec as P

LANES = 128
ROWS = 128
MESH = pl.DeviceIdType.MESH
F32 = jnp.float32
BF16 = jnp.bfloat16


def kernel(
    n_atom, n_tm, factor,
    signal_ref, spatial_ref, temporal_ref, values_ref, mask_ref,
    out_sp_ref, out_tm_ref,
    tail, halo, x, w, cbuf, ctbuf, sbuf, weights, own_w, sig, sig_t, proj, taps,
    sp_part, sp_recv, sp_full, tm_part, tm_recv, tm_full,
    halo_sems, s_send, s_recv, c_send, c_recv,
    sp_send, sp_rsem, sp_gsend, sp_grecv, tm_send, tm_rsem, tm_gsend, tm_grecv,
):
    atoms, channels = spatial_ref.shape
    length = temporal_ref.shape[1]
    samples = signal_ref.shape[1]
    blocks = mask_ref.shape[1]
    block = samples // blocks
    fold = LANES // atoms
    seg = samples // fold
    chunks = seg // ROWS
    share = atoms // n_tm
    me_a = lax.axis_index("atom")
    me_t = lax.axis_index("tm")
    a_peers = [lax.rem(me_a + d, n_atom) for d in range(1, n_atom)]
    t_peers = [lax.rem(me_t + d, n_tm) for d in range(1, n_tm)]

    barrier = pltpu.get_barrier_semaphore()
    for peer in a_peers:
        pl.semaphore_signal(barrier, inc=1, device_id={"atom": peer}, device_id_type=MESH)
    for peer in t_peers:
        pl.semaphore_signal(barrier, inc=1, device_id={"tm": peer}, device_id_type=MESH)

    mask = mask_ref[...].astype(F32)
    codes = jnp.concatenate(
        [
            values_ref[:, j * block : (j + 1) * block].astype(F32) * mask[:, j : j + 1]
            for j in range(blocks)
        ],
        axis=1,
    )
    tail[...] = codes[:, samples - length :].astype(BF16)

    pl.semaphore_wait(barrier, n_atom - 1 + n_tm - 1)

    right = lax.rem(me_t + 1, n_tm)
    halo_copy = pltpu.make_async_remote_copy(
        src_ref=tail, dst_ref=halo, send_sem=halo_sems.at[0], recv_sem=halo_sems.at[1],
        device_id={"tm": right}, device_id_type=MESH,
    )

    @pl.when(me_t < n_tm - 1)
    def _():
        halo_copy.start()

    s_copies = []
    for d, peer in enumerate(a_peers):
        copy = pltpu.make_async_remote_copy(
            src_ref=spatial_ref, dst_ref=sbuf.at[me_a], send_sem=s_send.at[d],
            recv_sem=s_recv.at[d], device_id={"atom": peer}, device_id_type=MESH,
        )
        copy.start()
        s_copies.append(copy)

    stacked = jnp.concatenate([codes[:, h * seg : (h + 1) * seg] for h in range(fold)], axis=0)
    x[length:, :] = stacked.T
    w[...] = jnp.concatenate([temporal_ref[...].astype(F32)] * fold, axis=0).T

    c_copies = [[None] * (n_atom - 1) for _ in range(chunks)]

    def convolve(c):
        base = length + c * ROWS

        def body(a, acc):
            for b in range(8):
                start = pl.multiple_of(base - 24 - 32 * a, 8) - b
                xs = x[pl.ds(start, ROWS + 24), :]
                for q in range(4):
                    tap = w[pl.ds(32 * a + 8 * q + b, 1), :]
                    acc = acc + xs[24 - 8 * q : 24 - 8 * q + ROWS] * tap
            return acc

        acc = lax.fori_loop(0, length // 32, body, jnp.zeros((ROWS, LANES), F32))
        course = acc.astype(BF16)
        rows = pl.ds(c * ROWS, ROWS)
        cbuf[me_a, rows, :] = course
        for d, peer in enumerate(a_peers):
            copy = pltpu.make_async_remote_copy(
                src_ref=cbuf.at[me_a, rows], dst_ref=cbuf.at[me_a, rows],
                send_sem=c_send.at[d, c], recv_sem=c_recv.at[d, c],
                device_id={"atom": peer}, device_id_type=MESH,
            )
            copy.start()
            c_copies[c][d] = copy
        ctbuf[c] = course.astype(F32).T.astype(BF16)

    late = [c for c in range(chunks) if c * ROWS >= length]
    early = [c for c in range(chunks) if c * ROWS < length]
    for c in late:
        convolve(c)

    @pl.when(me_t == 0)
    def _():
        halo[...] = jnp.zeros(halo.shape, halo.dtype)

    @pl.when(me_t > 0)
    def _():
        halo_copy.wait_recv()

    before = jnp.concatenate(
        [halo[...].astype(F32)] + [codes[:, h * seg - length : h * seg] for h in range(1, fold)],
        axis=0,
    )
    x[:length, :] = before.T
    for c in early:
        convolve(c)

    padded = sig.shape[0]
    sig[channels // 8 * 8 :, :] = jnp.zeros((padded - channels // 8 * 8, samples), F32)
    sig[:channels, :] = signal_ref[...].astype(F32)
    for c in range(samples // ROWS):
        sig_t[c * ROWS : (c + 1) * ROWS, :] = sig[:, c * ROWS : (c + 1) * ROWS].T

    sbuf[me_a] = spatial_ref[...]
    for copy in s_copies:
        copy.wait_recv()
    weights[...] = jnp.zeros(weights.shape, BF16)
    own_w[...] = jnp.zeros(own_w.shape, BF16)
    for h in range(fold):
        for g in range(n_atom):
            weights[h, g * LANES + h * atoms : g * LANES + (h + 1) * atoms, :channels] = sbuf[g]
        own_w[h, h * atoms : (h + 1) * atoms, :channels] = spatial_ref[...]

    gsp = None
    for c in late + early:
        for copy in c_copies[c]:
            copy.wait_recv()
        rows = slice(c * ROWS, (c + 1) * ROWS)
        lhs = jnp.concatenate([cbuf[g, rows, :] for g in range(n_atom)], axis=1)
        projected = None
        for h in range(fold):
            model = jnp.dot(lhs, weights[h], preferred_element_type=F32)
            at = h * seg + c * ROWS
            residual = (model - sig_t[at : at + ROWS, :]).astype(BF16)
            part = lax.dot_general(
                residual, own_w[h], (((1,), (1,)), ((), ())), preferred_element_type=F32
            )
            projected = part if projected is None else projected + part
            grad = jnp.dot(
                ctbuf[c, h * atoms : (h + 1) * atoms, :], residual, preferred_element_type=F32
            )
            gsp = grad if gsp is None else gsp + grad
        proj[rows, :] = projected.astype(BF16).astype(F32)

    def scatter(part, recv, send_sems, recv_sems):
        copies = []
        for d, peer in enumerate(t_peers):
            copy = pltpu.make_async_remote_copy(
                src_ref=part.at[peer], dst_ref=recv.at[d], send_sem=send_sems.at[d],
                recv_sem=recv_sems.at[d], device_id={"tm": peer}, device_id_type=MESH,
            )
            copy.start()
            copies.append(copy)
        return copies

    def gather(part, recv, full, copies, send_sems, recv_sems):
        total = part[me_t]
        for d, copy in enumerate(copies):
            copy.wait_recv()
            total = total + recv[d]
        full[me_t] = total * factor
        sent = []
        for d, peer in enumerate(t_peers):
            copy = pltpu.make_async_remote_copy(
                src_ref=full.at[me_t], dst_ref=full.at[me_t], send_sem=send_sems.at[d],
                recv_sem=recv_sems.at[d], device_id={"tm": peer}, device_id_type=MESH,
            )
            copy.start()
            sent.append(copy)
        return sent

    for j in range(n_tm):
        sp_part[j] = gsp[j * share : (j + 1) * share, :]
    sp_copies = scatter(sp_part, sp_recv, sp_send, sp_rsem)

    def correlate(lo, hi):
        def body(a, carry):
            for b in range(8):
                accs = [None] * 8
                for c in range(chunks):
                    p = proj[c * ROWS : (c + 1) * ROWS, :]
                    start = pl.multiple_of(length + c * ROWS - 56 - 64 * a, 8) - b
                    xs = x[pl.ds(start, ROWS + 56), :]
                    for q in range(8):
                        piece = p * xs[56 - 8 * q : 56 - 8 * q + ROWS]
                        for i in range(ROWS // 8):
                            row = piece[8 * i : 8 * i + 8]
                            accs[q] = row if accs[q] is None else accs[q] + row
                for q in range(8):
                    taps[pl.ds(64 * a + 8 * q + b, 1), :] = jnp.sum(accs[q], axis=0, keepdims=True)
            return carry

        lax.fori_loop(lo, hi, body, 0)

    halves = tm_part.shape[0]
    width = length // halves
    tm_copies = []
    sp_sent = None
    for half in range(halves):
        correlate(half * width // 64, (half + 1) * width // 64)
        if half == 0:
            sp_sent = gather(sp_part, sp_recv, sp_full, sp_copies, sp_gsend, sp_grecv)
        spread = taps[half * width : (half + 1) * width, :].T
        gtm = spread[:atoms]
        for h in range(1, fold):
            gtm = gtm + spread[h * atoms : (h + 1) * atoms]
        for j in range(n_tm):
            tm_part[half, j] = gtm[j * share : (j + 1) * share, :]
        tm_copies.append(
            scatter(tm_part.at[half], tm_recv.at[half], tm_send.at[half], tm_rsem.at[half])
        )
    tm_sent = []
    for half in range(halves):
        tm_sent.append(
            gather(
                tm_part.at[half], tm_recv.at[half], tm_full.at[half], tm_copies[half],
                tm_gsend.at[half], tm_grecv.at[half],
            )
        )

    for copy in sp_sent:
        copy.wait_recv()
    for j in range(n_tm):
        out_sp_ref[j * share : (j + 1) * share, :] = sp_full[j][:, :channels]
    for half in range(halves):
        for copy in tm_sent[half]:
            copy.wait_recv()
        for j in range(n_tm):
            out_tm_ref[j * share : (j + 1) * share, half * width : (half + 1) * width] = tm_full[half, j]

    @pl.when(me_t < n_tm - 1)
    def _():
        halo_copy.wait_send()

    for copy in s_copies + [copy for row in c_copies for copy in row]:
        copy.wait_send()
    for copy in sp_copies + sp_sent:
        copy.wait_send()
    for row in tm_copies + tm_sent:
        for copy in row:
            copy.wait_send()


def local(n_atom, n_tm, signal, spatial, temporal, values, mask):
    atoms, channels = spatial.shape
    length = temporal.shape[1]
    samples = signal.shape[1]
    fold = LANES // atoms
    seg = samples // fold
    chunks = seg // ROWS
    share = atoms // n_tm
    wide = -(-channels // LANES) * LANES
    halves = 2
    width = length // halves
    factor = 1.0 / math.sqrt(samples * n_tm)
    dma = pltpu.SemaphoreType.DMA
    vmem = pl.BlockSpec(memory_space=pltpu.VMEM)
    return pl.pallas_call(
        functools.partial(kernel, n_atom, n_tm, factor),
        out_shape=(
            jax.ShapeDtypeStruct((atoms, channels), F32),
            jax.ShapeDtypeStruct((atoms, length), F32),
        ),
        in_specs=[vmem] * 5,
        out_specs=(vmem, vmem),
        scratch_shapes=[
            pltpu.VMEM((atoms, length), BF16),
            pltpu.VMEM((atoms, length), BF16),
            pltpu.VMEM((length + seg, LANES), F32),
            pltpu.VMEM((length, LANES), F32),
            pltpu.VMEM((n_atom, seg, LANES), BF16),
            pltpu.VMEM((chunks, LANES, ROWS), BF16),
            pltpu.VMEM((n_atom, atoms, channels), BF16),
            pltpu.VMEM((fold, n_atom * LANES, wide), BF16),
            pltpu.VMEM((fold, LANES, wide), BF16),
            pltpu.VMEM((wide, samples), F32),
            pltpu.VMEM((samples, wide), F32),
            pltpu.VMEM((seg, LANES), F32),
            pltpu.VMEM((length, LANES), F32),
            pltpu.VMEM((n_tm, share, wide), F32),
            pltpu.VMEM((n_tm - 1, share, wide), F32),
            pltpu.VMEM((n_tm, share, wide), F32),
            pltpu.VMEM((halves, n_tm, share, width), F32),
            pltpu.VMEM((halves, n_tm - 1, share, width), F32),
            pltpu.VMEM((halves, n_tm, share, width), F32),
            dma((2,)),
            dma((n_atom - 1,)),
            dma((n_atom - 1,)),
            dma((n_atom - 1, chunks)),
            dma((n_atom - 1, chunks)),
            dma((n_tm - 1,)),
            dma((n_tm - 1,)),
            dma((n_tm - 1,)),
            dma((n_tm - 1,)),
            dma((halves, n_tm - 1)),
            dma((halves, n_tm - 1)),
            dma((halves, n_tm - 1)),
            dma((halves, n_tm - 1)),
        ],
        compiler_params=pltpu.CompilerParams(collective_id=0, has_side_effects=True),
    )(signal, spatial, temporal, values, mask)


def solution(mesh):
    in_specs = (P(None, "tm"), P("atom", None), P("atom", None), P("atom", "tm"), P("atom", "tm"))
    out_specs = (P("atom", None), P("atom", None))
    body = functools.partial(local, mesh.shape["atom"], mesh.shape["tm"])
    return jax.shard_map(body, mesh=mesh, in_specs=in_specs, out_specs=out_specs, check_vma=False)
```

```python
import functools
import math

import jax
import jax.numpy as jnp
from jax import lax
from jax.experimental import pallas as pl
from jax.experimental.pallas import tpu as pltpu
from jax.sharding import PartitionSpec as P

LANES = 128
ROWS = 128
MESH = pl.DeviceIdType.MESH
F32 = jnp.float32
BF16 = jnp.bfloat16


def kernel(
    n_atom, n_tm, factor,
    signal_ref, spatial_ref, temporal_ref, values_ref, mask_ref,
    out_sp_ref, out_tm_ref,
    tail, halo, x, w, cbuf, ctbuf, sbuf, weights, own_w, sig, sig_t, proj, sums, taps,
    sp_part, sp_recv, sp_full, tm_part, tm_recv, tm_full,
    halo_sems, s_send, s_recv, c_send, c_recv,
    sp_send, sp_rsem, sp_gsend, sp_grecv, tm_send, tm_rsem, tm_gsend, tm_grecv,
):
    atoms, channels = spatial_ref.shape
    length = temporal_ref.shape[1]
    samples = signal_ref.shape[1]
    blocks = mask_ref.shape[0]
    block = samples // blocks
    fold = LANES // atoms
    seg = samples // fold
    chunks = seg // ROWS
    share = atoms // n_tm
    me_a = lax.axis_index("atom")
    me_t = lax.axis_index("tm")
    a_peers = [lax.rem(me_a + d, n_atom) for d in range(1, n_atom)]
    t_peers = [lax.rem(me_t + d, n_tm) for d in range(1, n_tm)]

    barrier = pltpu.get_barrier_semaphore()
    for peer in a_peers:
        pl.semaphore_signal(barrier, inc=1, device_id={"atom": peer}, device_id_type=MESH)
    for peer in t_peers:
        pl.semaphore_signal(barrier, inc=1, device_id={"tm": peer}, device_id_type=MESH)

    mask = mask_ref[...].astype(F32).T
    codes = jnp.concatenate(
        [
            values_ref[:, j * block : (j + 1) * block].astype(F32) * mask[:, j : j + 1]
            for j in range(blocks)
        ],
        axis=1,
    )
    tail[...] = codes[:, samples - length :].astype(BF16)

    def enter():

        right = lax.rem(me_t + 1, n_tm)
        halo_copy = pltpu.make_async_remote_copy(
            src_ref=tail, dst_ref=halo, send_sem=halo_sems.at[0], recv_sem=halo_sems.at[1],
            device_id={"tm": right}, device_id_type=MESH,
        )

        @pl.when(me_t < n_tm - 1)
        def _():
            halo_copy.start()

        s_copies = []
        for d, peer in enumerate(a_peers):
            copy = pltpu.make_async_remote_copy(
                src_ref=spatial_ref, dst_ref=sbuf.at[me_a], send_sem=s_send.at[d],
                recv_sem=s_recv.at[d], device_id={"atom": peer}, device_id_type=MESH,
            )
            copy.start()
            s_copies.append(copy)
        return halo_copy, s_copies

    stacked = jnp.concatenate([codes[:, h * seg : (h + 1) * seg] for h in range(fold)], axis=0)
    x[length:, :] = stacked.T
    w[...] = jnp.concatenate([temporal_ref[...].astype(F32)] * fold, axis=0).T

    c_copies = [[None] * (n_atom - 1) for _ in range(chunks)]

    def convolve(c):
        base = length + c * ROWS

        def body(a, acc):
            for b in range(8):
                start = pl.multiple_of(base - 24 - 32 * a, 8) - b
                xs = x[pl.ds(start, ROWS + 24), :]
                for q in range(4):
                    tap = w[pl.ds(32 * a + 8 * q + b, 1), :]
                    acc = acc + xs[24 - 8 * q : 24 - 8 * q + ROWS] * tap
            return acc

        acc = lax.fori_loop(0, length // 32, body, jnp.zeros((ROWS, LANES), F32))
        course = acc.astype(BF16)
        rows = pl.ds(c * ROWS, ROWS)
        cbuf[me_a, rows, :] = course
        ctbuf[c] = course.astype(F32).T.astype(BF16)

    def send(c):
        rows = pl.ds(c * ROWS, ROWS)
        for d, peer in enumerate(a_peers):
            copy = pltpu.make_async_remote_copy(
                src_ref=cbuf.at[me_a, rows], dst_ref=cbuf.at[me_a, rows],
                send_sem=c_send.at[d, c], recv_sem=c_recv.at[d, c],
                device_id={"atom": peer}, device_id_type=MESH,
            )
            copy.start()
            c_copies[c][d] = copy

    late = [c for c in range(chunks) if c * ROWS >= length]
    early = [c for c in range(chunks) if c * ROWS < length]
    if not late:
        pl.semaphore_wait(barrier, n_atom - 1 + n_tm - 1)
        halo_copy, s_copies = enter()
    for i, c in enumerate(late):
        convolve(c)
        if i == 0:
            pl.semaphore_wait(barrier, n_atom - 1 + n_tm - 1)
            halo_copy, s_copies = enter()
        send(c)

    padded = sig.shape[0]
    sig[channels // 8 * 8 :, :] = jnp.zeros((padded - channels // 8 * 8, samples), F32)
    sig[:channels, :] = signal_ref[...].astype(F32)
    for c in range(samples // ROWS):
        sig_t[c * ROWS : (c + 1) * ROWS, :] = sig[:, c * ROWS : (c + 1) * ROWS].T

    @pl.when(me_t == 0)
    def _():
        halo[...] = jnp.zeros(halo.shape, halo.dtype)

    @pl.when(me_t > 0)
    def _():
        halo_copy.wait_recv()

    before = jnp.concatenate(
        [halo[...].astype(F32)] + [codes[:, h * seg - length : h * seg] for h in range(1, fold)],
        axis=0,
    )
    x[:length, :] = before.T
    for c in early:
        convolve(c)
        send(c)

    sbuf[me_a] = spatial_ref[...]
    for copy in s_copies:
        copy.wait_recv()
    weights[...] = jnp.zeros(weights.shape, BF16)
    own_w[...] = jnp.zeros(own_w.shape, BF16)
    for h in range(fold):
        for g in range(n_atom):
            weights[h, g * LANES + h * atoms : g * LANES + (h + 1) * atoms, :channels] = sbuf[g]
        own_w[h, h * atoms : (h + 1) * atoms, :channels] = spatial_ref[...]

    def process(c, gsp):
        for copy in c_copies[c]:
            copy.wait_recv()
        rows = slice(c * ROWS, (c + 1) * ROWS)
        lhs = jnp.concatenate([cbuf[g, rows, :] for g in range(n_atom)], axis=1)
        projected = None
        for h in range(fold):
            model = jnp.dot(lhs, weights[h], preferred_element_type=F32)
            at = h * seg + c * ROWS
            residual = (model - sig_t[at : at + ROWS, :]).astype(BF16)
            part = lax.dot_general(
                residual, own_w[h], (((1,), (1,)), ((), ())), preferred_element_type=F32
            )
            projected = part if projected is None else projected + part
            grad = jnp.dot(
                ctbuf[c, h * atoms : (h + 1) * atoms, :], residual, preferred_element_type=F32
            )
            gsp = grad if gsp is None else gsp + grad
        proj[rows, :] = projected.astype(BF16).astype(F32)
        return gsp

    def scatter(part, recv, send_sems, recv_sems):
        copies = []
        for d, peer in enumerate(t_peers):
            copy = pltpu.make_async_remote_copy(
                src_ref=part.at[peer], dst_ref=recv.at[d], send_sem=send_sems.at[d],
                recv_sem=recv_sems.at[d], device_id={"tm": peer}, device_id_type=MESH,
            )
            copy.start()
            copies.append(copy)
        return copies

    def gather(part, recv, full, copies, send_sems, recv_sems):
        total = part[me_t]
        for d, copy in enumerate(copies):
            copy.wait_recv()
            total = total + recv[d]
        full[me_t] = total * factor
        sent = []
        for d, peer in enumerate(t_peers):
            copy = pltpu.make_async_remote_copy(
                src_ref=full.at[me_t], dst_ref=full.at[me_t], send_sem=send_sems.at[d],
                recv_sem=recv_sems.at[d], device_id={"tm": peer}, device_id_type=MESH,
            )
            copy.start()
            sent.append(copy)
        return sent

    def correlate(c, lo, hi, first, last):
        def body(a, carry):
            p = proj[c * ROWS : (c + 1) * ROWS, :]
            for b in range(8):
                start = pl.multiple_of(length + c * ROWS - 56 - 64 * a, 8) - b
                xs = x[pl.ds(start, ROWS + 56), :]
                for q in range(8):
                    slot = pl.ds(pl.multiple_of(((a * 8 + b) * 8 + q) * 8, 8), 8)
                    acc = None if first else sums[slot, :]
                    piece = p * xs[56 - 8 * q : 56 - 8 * q + ROWS]
                    for i in range(ROWS // 8):
                        row = piece[8 * i : 8 * i + 8]
                        acc = row if acc is None else acc + row
                    if last:
                        tau = pl.ds(64 * a + 8 * q + b, 1)
                        taps[tau, :] = jnp.sum(acc, axis=0, keepdims=True)
                    else:
                        sums[slot, :] = acc
            return carry

        lax.fori_loop(lo, hi, body, 0)

    halves = tm_part.shape[0]
    width = length // halves
    steps = length // 64
    order = late + early
    near = order[: chunks // 2]
    gsp = None
    for c in near:
        gsp = process(c, gsp)
        correlate(c, 0, steps, c == order[0], False)
    for c in order[chunks // 2 :]:
        gsp = process(c, gsp)
    for j in range(n_tm):
        sp_part[j] = gsp[j * share : (j + 1) * share, :]
    sp_copies = scatter(sp_part, sp_recv, sp_send, sp_rsem)
    for c in order[chunks // 2 : -1]:
        correlate(c, 0, steps, c == order[0], False)
    tm_copies = []
    for half in range(halves):
        correlate(order[-1], half * width // 64, (half + 1) * width // 64, False, True)
        spread = taps[half * width : (half + 1) * width, :].T
        gtm = spread[:atoms]
        for h in range(1, fold):
            gtm = gtm + spread[h * atoms : (h + 1) * atoms]
        for j in range(n_tm):
            tm_part[half, j] = gtm[j * share : (j + 1) * share, :]
        tm_copies.append(
            scatter(tm_part.at[half], tm_recv.at[half], tm_send.at[half], tm_rsem.at[half])
        )
        if half == 0:
            sp_sent = gather(sp_part, sp_recv, sp_full, sp_copies, sp_gsend, sp_grecv)
    tm_sent = []
    for half in range(halves):
        tm_sent.append(
            gather(
                tm_part.at[half], tm_recv.at[half], tm_full.at[half], tm_copies[half],
                tm_gsend.at[half], tm_grecv.at[half],
            )
        )

    for copy in sp_sent:
        copy.wait_recv()
    for j in range(n_tm):
        out_sp_ref[j * share : (j + 1) * share, :] = sp_full[j][:, :channels]
    for half in range(halves):
        for copy in tm_sent[half]:
            copy.wait_recv()
        for j in range(n_tm):
            out_tm_ref[j * share : (j + 1) * share, half * width : (half + 1) * width] = tm_full[half, j]

    @pl.when(me_t < n_tm - 1)
    def _():
        halo_copy.wait_send()

    for copy in s_copies + [copy for row in c_copies for copy in row]:
        copy.wait_send()
    for copy in sp_copies + sp_sent:
        copy.wait_send()
    for row in tm_copies + tm_sent:
        for copy in row:
            copy.wait_send()


def local(n_atom, n_tm, signal, spatial, temporal, values, mask):
    atoms, channels = spatial.shape
    length = temporal.shape[1]
    samples = signal.shape[1]
    fold = LANES // atoms
    seg = samples // fold
    chunks = seg // ROWS
    share = atoms // n_tm
    wide = -(-channels // LANES) * LANES
    halves = 2
    width = length // halves
    factor = 1.0 / math.sqrt(samples * n_tm)
    dma = pltpu.SemaphoreType.DMA
    vmem = pl.BlockSpec(memory_space=pltpu.VMEM)
    return pl.pallas_call(
        functools.partial(kernel, n_atom, n_tm, factor),
        out_shape=(
            pltpu.VMEM((atoms, channels), F32),
            pltpu.VMEM((atoms, length), F32),
        ),
        in_specs=[vmem] * 5,
        out_specs=(vmem, vmem),
        scratch_shapes=[
            pltpu.VMEM((atoms, length), BF16),
            pltpu.VMEM((atoms, length), BF16),
            pltpu.VMEM((length + seg, LANES), F32),
            pltpu.VMEM((length, LANES), F32),
            pltpu.VMEM((n_atom, seg, LANES), BF16),
            pltpu.VMEM((chunks, LANES, ROWS), BF16),
            pltpu.VMEM((n_atom, atoms, channels), BF16),
            pltpu.VMEM((fold, n_atom * LANES, wide), BF16),
            pltpu.VMEM((fold, LANES, wide), BF16),
            pltpu.VMEM((wide, samples), F32),
            pltpu.VMEM((samples, wide), F32),
            pltpu.VMEM((seg, LANES), F32),
            pltpu.VMEM((8 * length, LANES), F32),
            pltpu.VMEM((length, LANES), F32),
            pltpu.VMEM((n_tm, share, wide), F32),
            pltpu.VMEM((n_tm - 1, share, wide), F32),
            pltpu.VMEM((n_tm, share, wide), F32),
            pltpu.VMEM((halves, n_tm, share, width), F32),
            pltpu.VMEM((halves, n_tm - 1, share, width), F32),
            pltpu.VMEM((halves, n_tm, share, width), F32),
            dma((2,)),
            dma((n_atom - 1,)),
            dma((n_atom - 1,)),
            dma((n_atom - 1, chunks)),
            dma((n_atom - 1, chunks)),
            dma((n_tm - 1,)),
            dma((n_tm - 1,)),
            dma((n_tm - 1,)),
            dma((n_tm - 1,)),
            dma((halves, n_tm - 1)),
            dma((halves, n_tm - 1)),
            dma((halves, n_tm - 1)),
            dma((halves, n_tm - 1)),
        ],
        compiler_params=pltpu.CompilerParams(collective_id=0, has_side_effects=True),
    )(signal, spatial, temporal, values, mask.T)


def solution(mesh):
    in_specs = (P(None, "tm"), P("atom", None), P("atom", None), P("atom", "tm"), P("atom", "tm"))
    out_specs = (P("atom", None), P("atom", None))
    body = functools.partial(local, mesh.shape["atom"], mesh.shape["tm"])
    return jax.shard_map(body, mesh=mesh, in_specs=in_specs, out_specs=out_specs, check_vma=False)
```

```python
import functools
import math

import jax
import jax.numpy as jnp
from jax import lax
from jax.experimental import pallas as pl
from jax.experimental.pallas import tpu as pltpu
from jax.sharding import PartitionSpec as P

LANES = 128
ROWS = 128
MESH = pl.DeviceIdType.MESH
F32 = jnp.float32
BF16 = jnp.bfloat16


def kernel(
    n_atom, n_tm, factor,
    signal_ref, spatial_ref, temporal_ref, values_ref, mask_ref,
    out_sp_ref, out_tm_ref,
    tail, halo, x, w, cbuf, ctbuf, sbuf, weights, own_w, sig, sig_t, proj, sums, taps,
    sp_part, sp_recv, sp_full, tm_part, tm_recv, tm_full,
    halo_sems, s_send, s_recv, c_send, c_recv,
    sp_send, sp_rsem, sp_gsend, sp_grecv, tm_send, tm_rsem, tm_gsend, tm_grecv,
):
    atoms, channels = spatial_ref.shape
    length = temporal_ref.shape[1]
    samples = signal_ref.shape[1]
    blocks = mask_ref.shape[0]
    block = samples // blocks
    fold = LANES // atoms
    seg = samples // fold
    chunks = seg // ROWS
    share = atoms // n_tm
    me_a = lax.axis_index("atom")
    me_t = lax.axis_index("tm")
    a_peers = [lax.rem(me_a + d, n_atom) for d in range(1, n_atom)]
    t_peers = [lax.rem(me_t + d, n_tm) for d in range(1, n_tm)]

    barrier = pltpu.get_barrier_semaphore()
    for peer in a_peers:
        pl.semaphore_signal(barrier, inc=1, device_id={"atom": peer}, device_id_type=MESH)
    for peer in t_peers:
        pl.semaphore_signal(barrier, inc=1, device_id={"tm": peer}, device_id_type=MESH)

    mask = mask_ref[...].astype(F32).T
    codes = jnp.concatenate(
        [
            values_ref[:, j * block : (j + 1) * block].astype(F32) * mask[:, j : j + 1]
            for j in range(blocks)
        ],
        axis=1,
    )
    tail[...] = codes[:, samples - length :].astype(BF16)

    def enter():

        right = lax.rem(me_t + 1, n_tm)
        halo_copy = pltpu.make_async_remote_copy(
            src_ref=tail, dst_ref=halo, send_sem=halo_sems.at[0], recv_sem=halo_sems.at[1],
            device_id={"tm": right}, device_id_type=MESH,
        )

        @pl.when(me_t < n_tm - 1)
        def _():
            halo_copy.start()

        s_copies = []
        for d, peer in enumerate(a_peers):
            copy = pltpu.make_async_remote_copy(
                src_ref=spatial_ref, dst_ref=sbuf.at[me_a], send_sem=s_send.at[d],
                recv_sem=s_recv.at[d], device_id={"atom": peer}, device_id_type=MESH,
            )
            copy.start()
            s_copies.append(copy)
        return halo_copy, s_copies

    stacked = jnp.concatenate([codes[:, h * seg : (h + 1) * seg] for h in range(fold)], axis=0)
    x[length:, :] = stacked.T
    w[...] = jnp.concatenate([temporal_ref[...].astype(F32)] * fold, axis=0).T

    c_copies = [[None] * (n_atom - 1) for _ in range(chunks)]

    def convolve(c):
        base = length + c * ROWS

        def body(a, acc):
            for b in range(8):
                start = pl.multiple_of(base - 24 - 32 * a, 8) - b
                xs = x[pl.ds(start, ROWS + 24), :]
                for q in range(4):
                    tap = w[pl.ds(32 * a + 8 * q + b, 1), :]
                    acc = acc + xs[24 - 8 * q : 24 - 8 * q + ROWS] * tap
            return acc

        acc = lax.fori_loop(0, length // 32, body, jnp.zeros((ROWS, LANES), F32))
        course = acc.astype(BF16)
        rows = pl.ds(c * ROWS, ROWS)
        cbuf[me_a, rows, :] = course
        ctbuf[c] = course.astype(F32).T.astype(BF16)

    def send(c):
        rows = pl.ds(c * ROWS, ROWS)
        for d, peer in enumerate(a_peers):
            copy = pltpu.make_async_remote_copy(
                src_ref=cbuf.at[me_a, rows], dst_ref=cbuf.at[me_a, rows],
                send_sem=c_send.at[d, c], recv_sem=c_recv.at[d, c],
                device_id={"atom": peer}, device_id_type=MESH,
            )
            copy.start()
            c_copies[c][d] = copy

    late = [c for c in range(chunks) if c * ROWS >= length]
    early = [c for c in range(chunks) if c * ROWS < length]
    if not late:
        pl.semaphore_wait(barrier, n_atom - 1 + n_tm - 1)
        halo_copy, s_copies = enter()
    for i, c in enumerate(late):
        convolve(c)
        if i == 0:
            pl.semaphore_wait(barrier, n_atom - 1 + n_tm - 1)
            halo_copy, s_copies = enter()
        send(c)

    padded = sig.shape[0]
    sig[channels // 8 * 8 :, :] = jnp.zeros((padded - channels // 8 * 8, samples), F32)
    sig[:channels, :] = signal_ref[...].astype(F32)
    for c in range(samples // ROWS):
        sig_t[c * ROWS : (c + 1) * ROWS, :] = sig[:, c * ROWS : (c + 1) * ROWS].T

    @pl.when(me_t == 0)
    def _():
        halo[...] = jnp.zeros(halo.shape, halo.dtype)

    @pl.when(me_t > 0)
    def _():
        halo_copy.wait_recv()

    before = jnp.concatenate(
        [halo[...].astype(F32)] + [codes[:, h * seg - length : h * seg] for h in range(1, fold)],
        axis=0,
    )
    x[:length, :] = before.T
    for c in early:
        convolve(c)
        send(c)

    sbuf[me_a] = spatial_ref[...]
    for copy in s_copies:
        copy.wait_recv()
    weights[...] = jnp.zeros(weights.shape, BF16)
    own_w[...] = jnp.zeros(own_w.shape, BF16)
    for h in range(fold):
        for g in range(n_atom):
            weights[h, g * LANES + h * atoms : g * LANES + (h + 1) * atoms, :channels] = sbuf[g]
        own_w[h, h * atoms : (h + 1) * atoms, :channels] = spatial_ref[...]

    def process(c, gsp):
        for copy in c_copies[c]:
            copy.wait_recv()
        rows = slice(c * ROWS, (c + 1) * ROWS)
        lhs = jnp.concatenate([cbuf[g, rows, :] for g in range(n_atom)], axis=1)
        projected = None
        for h in range(fold):
            model = jnp.dot(lhs, weights[h], preferred_element_type=F32)
            at = h * seg + c * ROWS
            residual = (model - sig_t[at : at + ROWS, :]).astype(BF16)
            part = lax.dot_general(
                residual, own_w[h], (((1,), (1,)), ((), ())), preferred_element_type=F32
            )
            projected = part if projected is None else projected + part
            grad = jnp.dot(
                ctbuf[c, h * atoms : (h + 1) * atoms, :], residual, preferred_element_type=F32
            )
            gsp = grad if gsp is None else gsp + grad
        proj[rows, :] = projected.astype(BF16).astype(F32)
        return gsp

    def scatter(part, recv, send_sems, recv_sems):
        copies = []
        for d, peer in enumerate(t_peers):
            copy = pltpu.make_async_remote_copy(
                src_ref=part.at[peer], dst_ref=recv.at[d], send_sem=send_sems.at[d],
                recv_sem=recv_sems.at[d], device_id={"tm": peer}, device_id_type=MESH,
            )
            copy.start()
            copies.append(copy)
        return copies

    def gather(part, recv, full, copies, send_sems, recv_sems):
        total = part[me_t]
        for d, copy in enumerate(copies):
            copy.wait_recv()
            total = total + recv[d]
        full[me_t] = total * factor
        sent = []
        for d, peer in enumerate(t_peers):
            copy = pltpu.make_async_remote_copy(
                src_ref=full.at[me_t], dst_ref=full.at[me_t], send_sem=send_sems.at[d],
                recv_sem=recv_sems.at[d], device_id={"tm": peer}, device_id_type=MESH,
            )
            copy.start()
            sent.append(copy)
        return sent

    def correlate(c, lo, hi, first, last):
        def body(a, carry):
            p = proj[c * ROWS : (c + 1) * ROWS, :]
            for b in range(8):
                start = pl.multiple_of(length + c * ROWS - 56 - 64 * a, 8) - b
                xs = x[pl.ds(start, ROWS + 56), :]
                for q in range(8):
                    slot = pl.ds(pl.multiple_of(((a * 8 + b) * 8 + q) * 8, 8), 8)
                    acc = None if first else sums[slot, :]
                    piece = p * xs[56 - 8 * q : 56 - 8 * q + ROWS]
                    for i in range(ROWS // 8):
                        row = piece[8 * i : 8 * i + 8]
                        acc = row if acc is None else acc + row
                    if last:
                        tau = pl.ds(64 * a + 8 * q + b, 1)
                        taps[tau, :] = jnp.sum(acc, axis=0, keepdims=True)
                    else:
                        sums[slot, :] = acc
            return carry

        lax.fori_loop(lo, hi, body, 0)

    halves = tm_part.shape[0]
    width = length // halves
    steps = length // 64
    order = late + early
    near = order[: chunks // 2]
    gsp = None
    for c in near:
        gsp = process(c, gsp)
        correlate(c, 0, steps, c == order[0], False)
    for c in order[chunks // 2 :]:
        gsp = process(c, gsp)
    for j in range(n_tm):
        sp_part[j] = gsp[j * share : (j + 1) * share, :]
    sp_copies = scatter(sp_part, sp_recv, sp_send, sp_rsem)
    for c in order[chunks // 2 : -1]:
        correlate(c, 0, steps, c == order[0], False)
    tm_copies = []
    for half in range(halves):
        correlate(order[-1], half * width // 64, (half + 1) * width // 64, False, True)
        spread = taps[half * width : (half + 1) * width, :].T
        gtm = spread[:atoms]
        for h in range(1, fold):
            gtm = gtm + spread[h * atoms : (h + 1) * atoms]
        for j in range(n_tm):
            tm_part[half, j] = gtm[j * share : (j + 1) * share, :]
        tm_copies.append(
            scatter(tm_part.at[half], tm_recv.at[half], tm_send.at[half], tm_rsem.at[half])
        )
        if half == 0:
            sp_sent = gather(sp_part, sp_recv, sp_full, sp_copies, sp_gsend, sp_grecv)
    tm_sent = []
    for half in range(halves):
        tm_sent.append(
            gather(
                tm_part.at[half], tm_recv.at[half], tm_full.at[half], tm_copies[half],
                tm_gsend.at[half], tm_grecv.at[half],
            )
        )

    for copy in sp_sent:
        copy.wait_recv()
    for j in range(n_tm):
        out_sp_ref[j * share : (j + 1) * share, :] = sp_full[j][:, :channels]
    for half in range(halves):
        for copy in tm_sent[half]:
            copy.wait_recv()
        for j in range(n_tm):
            out_tm_ref[j * share : (j + 1) * share, half * width : (half + 1) * width] = tm_full[half, j]

    @pl.when(me_t < n_tm - 1)
    def _():
        halo_copy.wait_send()

    for copy in s_copies + [copy for row in c_copies for copy in row]:
        copy.wait_send()
    for copy in sp_copies + sp_sent:
        copy.wait_send()
    for row in tm_copies + tm_sent:
        for copy in row:
            copy.wait_send()


def local(n_atom, n_tm, signal, spatial, temporal, values, mask):
    atoms, channels = spatial.shape
    length = temporal.shape[1]
    samples = signal.shape[1]
    fold = LANES // atoms
    seg = samples // fold
    chunks = seg // ROWS
    share = atoms // n_tm
    wide = -(-channels // LANES) * LANES
    halves = 1
    width = length // halves
    factor = 1.0 / math.sqrt(samples * n_tm)
    dma = pltpu.SemaphoreType.DMA
    vmem = pl.BlockSpec(memory_space=pltpu.VMEM)
    return pl.pallas_call(
        functools.partial(kernel, n_atom, n_tm, factor),
        out_shape=(
            pltpu.VMEM((atoms, channels), F32),
            pltpu.VMEM((atoms, length), F32),
        ),
        in_specs=[vmem] * 5,
        out_specs=(vmem, vmem),
        scratch_shapes=[
            pltpu.VMEM((atoms, length), BF16),
            pltpu.VMEM((atoms, length), BF16),
            pltpu.VMEM((length + seg, LANES), F32),
            pltpu.VMEM((length, LANES), F32),
            pltpu.VMEM((n_atom, seg, LANES), BF16),
            pltpu.VMEM((chunks, LANES, ROWS), BF16),
            pltpu.VMEM((n_atom, atoms, channels), BF16),
            pltpu.VMEM((fold, n_atom * LANES, wide), BF16),
            pltpu.VMEM((fold, LANES, wide), BF16),
            pltpu.VMEM((wide, samples), F32),
            pltpu.VMEM((samples, wide), F32),
            pltpu.VMEM((seg, LANES), F32),
            pltpu.VMEM((8 * length, LANES), F32),
            pltpu.VMEM((length, LANES), F32),
            pltpu.VMEM((n_tm, share, wide), F32),
            pltpu.VMEM((n_tm - 1, share, wide), F32),
            pltpu.VMEM((n_tm, share, wide), F32),
            pltpu.VMEM((halves, n_tm, share, width), F32),
            pltpu.VMEM((halves, n_tm - 1, share, width), F32),
            pltpu.VMEM((halves, n_tm, share, width), F32),
            dma((2,)),
            dma((n_atom - 1,)),
            dma((n_atom - 1,)),
            dma((n_atom - 1, chunks)),
            dma((n_atom - 1, chunks)),
            dma((n_tm - 1,)),
            dma((n_tm - 1,)),
            dma((n_tm - 1,)),
            dma((n_tm - 1,)),
            dma((halves, n_tm - 1)),
            dma((halves, n_tm - 1)),
            dma((halves, n_tm - 1)),
            dma((halves, n_tm - 1)),
        ],
        compiler_params=pltpu.CompilerParams(collective_id=0, has_side_effects=True),
    )(signal, spatial, temporal, values, mask.T)


def solution(mesh):
    in_specs = (P(None, "tm"), P("atom", None), P("atom", None), P("atom", "tm"), P("atom", "tm"))
    out_specs = (P("atom", None), P("atom", None))
    body = functools.partial(local, mesh.shape["atom"], mesh.shape["tm"])
    return jax.shard_map(body, mesh=mesh, in_specs=in_specs, out_specs=out_specs, check_vma=False)
```
